128 devices in a mesh: dp: 8 (over x, y_lo), vocab: 16 (over z, y_hi, core).
Axes of the slice: x: 4, y: 4 (y_hi: 2, y_lo: 2; y = y_hi * 2 + y_lo), z: 4, core: 2. Of those that a mesh axis runs over, the one named last changes fastest.
Arguments:
- hidden: bfloat16 [8192, 5120], P(('dp', 'vocab')), may hold values from -100 to 100
- tokens: int32 [8192], P('dp'), may hold values from 0 to 18431
- old_weight: bfloat16 [18432, 5120], P('vocab'), may hold values from -1 to 1
- new_weight: bfloat16 [18432, 5120], P('dp', 'vocab'), may hold values from -6 to 6
Outputs:
- logprob: float32 [8192], P(('dp', 'vocab'))
- engine_weight: bfloat16 [18432, 5120], P('vocab')
The draws below stay inside these ranges and needn't reach their ends.
All inputs are finite; a program needn't handle non-finite values.
Results may differ from the reference program's by a relative error of at most 0.001.
Values may be sent and summed in bfloat16 or wider, within the bound.
No kernel may reach another device: no remote copies, remote signals or barrier semaphores. Data moves between devices by JAX's collectives and lax.ppermute only.
A program may use at most 128 MiB of HBM per device.

```python
import math
import jax
import jax.numpy as jnp
from jax import lax

D = 5120
VOCAB = 18432
GROUP_ROWS = 1024
ROWS = 8192
N_DP = 8


def base_weight(key):
    first_key = jax.random.fold_in(jax.random.fold_in(key, 11), 0)
    weights = jax.random.normal(first_key, (VOCAB, D), jnp.float32) / math.sqrt(D)
    return jnp.clip(weights, -1.0, 1.0)


def draw_old_weight(key, part):
    return base_weight(key).astype(jnp.bfloat16)


def draw_hidden(key, part):
    keys = jax.random.split(jax.random.fold_in(key, 23), 1)
    values = 3.0 * jax.random.normal(keys[0], (ROWS, D), jnp.float32)
    return jnp.clip(values, -100.0, 100.0).astype(jnp.bfloat16)


def set_ends(array, own_key, smallest, high):
    spot = [jax.random.randint(jax.random.fold_in(own_key, axis), (), 0, length) for axis, length in enumerate(array.shape)]
    longest = array.shape.index(max(array.shape))
    neighbour = spot[:longest] + [(spot[longest] + 1) % array.shape[longest]] + spot[longest + 1:]
    return array.at[tuple(spot)].set(smallest).at[tuple(neighbour)].set(high)


def levels(stream_key, shape, shards, least, top_value):
    gain = 1.0
    for position, shards_of in shards:
        steps = jax.random.uniform(jax.random.fold_in(jax.random.fold_in(stream_key, 6), position), (shards_of,), jnp.float32, least / len(shards), top_value / len(shards))
        gain = gain * jnp.repeat(jnp.exp(steps), shape[position] // shards_of).reshape((-1,) + (1,) * (len(shape) - 1 - position))
    return gain


def bell_draw(key, shape, deviation, bound, shards=(), dtype=jnp.bfloat16):
    result = deviation * jax.random.normal(key, shape, jnp.float32)
    if shards:
        result = result * levels(key, shape, shards, -0.22, 0.18)
    return jnp.clip(result, -bound, bound).astype(dtype)


def setup_inputs(seed: int = 0) -> dict:
    key_of = jax.random.split(jax.random.key(seed), 5)
    hidden = draw_hidden(jax.random.fold_in(key_of[4], 71), 0)
    tokens = set_ends(jax.random.randint(key_of[1], (ROWS,), 0, VOCAB), jax.random.fold_in(key_of[1], 1), 0, VOCAB - 1).astype(jnp.int32)
    old_weight = draw_old_weight(jax.random.fold_in(key_of[4], 71), 0)
    new_weight = bell_draw(key_of[3], (VOCAB, D), 1.0, 6.0, ((0, 8), (1, 16)))
    return dict(hidden=hidden, tokens=tokens, old_weight=old_weight, new_weight=new_weight)


def reference(hidden, tokens, old_weight, new_weight):
    def one_group(operands):
        rows, ids = operands
        logits = jnp.dot(rows, old_weight.T, preferred_element_type=jnp.float32)
        top = jnp.max(logits, axis=1)
        total = jnp.sum(jnp.exp(logits - top[:, None]), axis=1)
        target = jnp.take_along_axis(logits, ids[:, None].astype(jnp.int32), axis=1)[:, 0]
        return target - top - jnp.log(total)

    grouped = hidden.reshape(N_DP, GROUP_ROWS, D)
    grouped_ids = tokens.reshape(N_DP, GROUP_ROWS)
    logprob = lax.map(one_group, (grouped, grouped_ids)).reshape(ROWS)
    return logprob, new_weight
```

```python
import jax
import jax.numpy as jnp
from jax import lax
from jax.experimental import pallas as pl
from jax.experimental.pallas import tpu as pltpu
from jax.sharding import Mesh
from jax.sharding import PartitionSpec as P

AXES = ("x", "q", "z", "h", "k")
SIZES = (4, 2, 4, 2, 2)
CHUNK = 288
ROWS_A = 176


def place(x, q, z, h, k):
    return (((x * 2 + q) * 4 + z) * 2 + h) * 2 + k


def pairs(move):
    found = []
    for x in range(4):
        for q in range(2):
            for z in range(4):
                for h in range(2):
                    for k in range(2):
                        found.append((place(x, q, z, h, k), place(*move(x, q, z, h, k))))
    return found


def send(value, move):
    return lax.ppermute(value, AXES, pairs(move))


def swap_core(value):
    return send(value, lambda x, q, z, h, k: (x, q, z, h, 1 - k))


def swap_q(value):
    return send(value, lambda x, q, z, h, k: (x, 1 - q, z, h, k))


def swap_h(value):
    return send(value, lambda x, q, z, h, k: (x, q, z, 1 - h, k))


def along_z(value, step):
    return send(value, lambda x, q, z, h, k: (x, q, (z + step) % 4, h, k))


def along_x(value, step):
    return send(value, lambda x, q, z, h, k: ((x + step) % 4, q, z, h, k))


def to_owner(value, step):
    return send(value, lambda x, q, z, h, k: ((z + step) % 4, (h + step // 2) % 2, x, q, k))


def turn_kernel(where_ref, own_ref, got_ref, *refs):
    outs, scratch = refs[:4], refs[4]
    own, got = own_ref[...], got_ref[...]
    first = where_ref[0] == 0
    both = jnp.concatenate([jnp.where(first, own, got), jnp.where(first, got, own)], axis=0)
    scratch[...] = both.T
    for step in range(4):
        start = pl.multiple_of(((where_ref[1] + step) % 4) * CHUNK, 32)
        outs[step][...] = scratch[pl.ds(start, CHUNK), :]


def turn(where, turned, got):
    width, rows = got.shape
    return pl.pallas_call(
        turn_kernel,
        out_shape=[jax.ShapeDtypeStruct((CHUNK, 2 * width), got.dtype)] * 4,
        grid_spec=pltpu.PrefetchScalarGridSpec(
            num_scalar_prefetch=1,
            grid=(1,),
            in_specs=[
                pl.BlockSpec((width, rows), lambda i, where: (0, where[0])),
                pl.BlockSpec((width, rows), lambda i, where: (0, 0)),
            ],
            out_specs=[pl.BlockSpec((CHUNK, 2 * width), lambda i, where: (0, 0))] * 4,
            scratch_shapes=[pltpu.VMEM((rows, 2 * width), got.dtype)],
        ),
        name="turn",
    )(where, turned, got)


def laid(spots):
    def kernel(where_ref, *refs):
        count = len(spots)
        blocks, stages = refs[:count], refs[-count - 2 : -2]
        out_ref, into, out_of = refs[-count - 3], refs[-2], refs[-1]
        loads = [
            pltpu.make_async_copy(block, stage, into.at[i]) for i, (block, stage) in enumerate(zip(blocks, stages))
        ]
        for load in loads:
            load.start()
        stores = []
        for load, stage, (dx, other, steps, first) in zip(loads, stages, spots):
            load.wait()
            source = (where_ref[0] + dx) % 4
            rows = stage.shape[1]
            for at, step in enumerate(steps):
                h = (where_ref[1] + other + step // 2) % 2
                column = ((source - step + 4) % 4 * 2 + h) * 640
                row = source * CHUNK + first
                store = pltpu.make_async_copy(
                    stage.at[at],
                    out_ref.at[pl.ds(pl.multiple_of(row, 16), rows), pl.ds(pl.multiple_of(column, 128), 640)],
                    out_of.at[len(stores)],
                )
                store.start()
                stores.append(store)
        for store in stores:
            store.wait()

    return kernel


def lay(where, blocks, spots, into=None):
    count = sum(len(spot[2]) for spot in spots)
    anywhere = pl.BlockSpec(memory_space=pl.ANY)
    operands = list(blocks) + ([] if into is None else [into])
    return pl.pallas_call(
        laid(spots),
        out_shape=jax.ShapeDtypeStruct((4 * CHUNK, 5120), blocks[0].dtype),
        grid_spec=pltpu.PrefetchScalarGridSpec(
            num_scalar_prefetch=1,
            grid=(1,),
            in_specs=[anywhere] * len(operands),
            out_specs=anywhere,
            scratch_shapes=[pltpu.VMEM(block.shape, block.dtype) for block in blocks]
            + [pltpu.SemaphoreType.DMA((len(blocks),)), pltpu.SemaphoreType.DMA((count,))],
        ),
        input_output_aliases={} if into is None else {len(operands): 0},
        name="lay",
    )(where, *operands)


def first_moves(new_weight):
    rows = new_weight.shape[0] // 2
    z, core = lax.axis_index("z"), lax.axis_index("k")
    turned = new_weight.T
    other = lax.dynamic_slice(turned, (0, (1 - core) * rows), (turned.shape[0], rows))
    chunks = turn(jnp.stack([core, z]).astype(jnp.int32), turned, swap_core(other))
    got = [to_owner(chunks[step], step) for step in range(4)]
    own_a = jnp.stack([block[:ROWS_A] for block in got])
    own_b = jnp.stack([block[ROWS_A:] for block in got])
    return own_a, own_b


def move_weight(own_a, own_b):
    x, q = lax.axis_index("x"), lax.axis_index("q")
    ya = swap_q(own_a)
    a_m, a_p = along_x(own_a, 1), along_x(own_a, -1)
    yb = swap_q(own_b)
    b_m, b_p = along_x(own_b, 1), along_x(own_b, -1)
    a_2 = along_x(a_m, 1)
    b_2 = along_x(b_p, -1)
    ya_m, ya_p = along_x(ya, 1), along_x(ya, -1)
    ya_2 = along_x(ya_p, -1)
    yb_m = swap_q(b_m)
    yb_p = swap_q(b_p)
    yb_2 = swap_q(b_2)
    four = (0, 1, 2, 3)
    where = jnp.stack([x, q]).astype(jnp.int32)
    out = lay(
        where,
        [own_a, own_b, a_m, a_p, b_m, b_p, ya, yb],
        [
            (0, 0, four, 0),
            (0, 0, four, ROWS_A),
            (3, 0, four, 0),
            (1, 0, four, 0),
            (3, 0, four, ROWS_A),
            (1, 0, four, ROWS_A),
            (0, 1, four, 0),
            (0, 1, four, ROWS_A),
        ],
    )
    return lay(
        where,
        [a_2, b_2, ya_m, ya_p, yb_m, yb_p, ya_2, yb_2],
        [
            (2, 0, four, 0),
            (2, 0, four, ROWS_A),
            (3, 1, four, 0),
            (1, 1, four, 0),
            (3, 1, four, ROWS_A),
            (1, 1, four, ROWS_A),
            (2, 1, four, 0),
            (2, 1, four, ROWS_A),
        ],
        out,
    )


def stats_kernel(ids_ref, near_ref, far_ref, weight_ref, out_ref, rows_ref, sems):
    step = pl.program_id(0)
    half = near_ref.shape[0]

    @pl.when(step == 0)
    def _():
        copies = [
            pltpu.make_async_copy(near_ref, rows_ref.at[pl.ds(0, half)], sems.at[0]),
            pltpu.make_async_copy(far_ref, rows_ref.at[pl.ds(half, half)], sems.at[1]),
        ]
        for copy in copies:
            copy.start()
        for copy in copies:
            copy.wait()

    logits = lax.dot_general(
        weight_ref[...], rows_ref[...], (((1,), (1,)), ((), ())), preferred_element_type=jnp.float32
    )
    ids = lax.broadcasted_iota(jnp.int32, logits.shape, 0) + step * logits.shape[0]
    found = jnp.sum(jnp.where(ids == ids_ref[...], logits, 0.0), axis=0, keepdims=True)
    top = jnp.max(logits, axis=0, keepdims=True)

    @pl.when(step == 0)
    def _():
        out_ref[0:1] = top
        out_ref[1:2] = jnp.sum(jnp.exp(logits - top), axis=0, keepdims=True)
        out_ref[2:3] = found

    @pl.when(step > 0)
    def _():
        before = out_ref[0:1]
        highest = jnp.maximum(before, top)
        summed = jnp.sum(jnp.exp(logits - highest), axis=0, keepdims=True)
        out_ref[0:1] = highest
        out_ref[1:2] = out_ref[1:2] * jnp.exp(before - highest) + summed
        out_ref[2:3] = out_ref[2:3] + found


def part_stats(near, far, weight, ids):
    count = 2 * near.shape[0]
    tile = 384
    anywhere = pl.BlockSpec(memory_space=pl.ANY)
    return pl.pallas_call(
        stats_kernel,
        out_shape=jax.ShapeDtypeStruct((3, count), jnp.float32),
        grid=(weight.shape[0] // tile,),
        in_specs=[
            pl.BlockSpec((1, count), lambda i: (0, 0)),
            anywhere,
            anywhere,
            pl.BlockSpec((tile, weight.shape[1]), lambda i: (i, 0)),
        ],
        out_specs=pl.BlockSpec((3, count), lambda i: (0, 0)),
        scratch_shapes=[pltpu.VMEM((count, weight.shape[1]), near.dtype), pltpu.SemaphoreType.DMA((2,))],
        name="stats",
    )(ids.reshape(1, count), near, far, weight)


def by_owner(stats):
    z, h, k = lax.axis_index("z"), lax.axis_index("h"), lax.axis_index("k")
    stats = stats[::-1]
    stats = jnp.concatenate([stats, stats], axis=0)
    stats = lax.dynamic_slice_in_dim(stats, (3 - z) % 4, 4, axis=0)
    stats = jnp.where(h == 0, stats, stats[:, ::-1])
    return jnp.where(k == 0, stats, stats[:, :, ::-1])


def relative(owned):
    z, h, k = lax.axis_index("z"), lax.axis_index("h"), lax.axis_index("k")
    owned = jnp.where(k == 0, owned, owned[:, :, ::-1])
    owned = jnp.where(h == 0, owned, owned[:, ::-1])
    owned = owned[::-1]
    owned = jnp.concatenate([owned, owned], axis=0)
    return lax.dynamic_slice_in_dim(owned, (3 - z) % 4, 4, axis=0)


def log_probs(hidden, tokens, old_weight):
    own_rows = hidden.shape[0]
    rank = (lax.axis_index("z") * 2 + lax.axis_index("h")) * 2 + lax.axis_index("k")
    wanted = relative(tokens.reshape(4, 2, 2, own_rows)) - rank * old_weight.shape[0]
    m, p = along_z(hidden, 1), along_z(hidden, -1)
    flipped = swap_h(hidden)
    far = along_z(m, 1)
    groups = [jnp.concatenate([hidden, m, far, p], axis=0)]
    m, p = along_z(flipped, 1), along_z(flipped, -1)
    far = along_z(p, -1)
    groups.append(jnp.concatenate([flipped, m, far, p], axis=0))
    stats = []
    for flip, group in enumerate(groups):
        ids = wanted[:, flip].transpose(1, 0, 2).reshape(-1)
        stats.append(part_stats(group, swap_core(group), old_weight, ids).reshape(3, 2, 4, own_rows))
    stats = jnp.stack(stats, axis=0).transpose(3, 0, 2, 1, 4)
    stats = by_owner(stats).reshape(16, 3 * own_rows)
    stats = lax.all_to_all(stats, ("z", "h", "k"), split_axis=0, concat_axis=0, tiled=True)
    stats = stats.reshape(16, 3, own_rows)
    highest = jnp.max(stats[:, 0], axis=0)
    summed = jnp.sum(stats[:, 1] * jnp.exp(stats[:, 0] - highest[None, :]), axis=0)
    target = jnp.sum(stats[:, 2], axis=0)
    return target - highest - jnp.log(summed)


def on_device(hidden, tokens, old_weight, new_weight):
    own_a, own_b = first_moves(new_weight)
    return log_probs(hidden, tokens, old_weight), move_weight(own_a, own_b)


def solution(mesh):
    finer = Mesh(mesh.devices.reshape(SIZES), AXES)
    return jax.shard_map(
        on_device,
        mesh=finer,
        in_specs=(P(AXES, None), P(("x", "q")), P(("z", "h", "k"), None), P(("x", "q"), ("z", "h", "k"))),
        out_specs=(P(AXES), P(("z", "h", "k"), None)),
        check_vma=False,
    )
```

```python
import jax
import jax.numpy as jnp
from jax import lax
from jax.experimental import pallas as pl
from jax.experimental.pallas import tpu as pltpu
from jax.sharding import Mesh
from jax.sharding import PartitionSpec as P

AXES = ("x", "q", "z", "h", "k")
SIZES = (4, 2, 4, 2, 2)
TILE = 384
TILE = 384
STATS_VMEM = 56
CHUNK = 288


def place(x, q, z, h, k):
    return (((x * 2 + q) * 4 + z) * 2 + h) * 2 + k


def pairs(move):
    found = []
    for x in range(4):
        for q in range(2):
            for z in range(4):
                for h in range(2):
                    for k in range(2):
                        found.append((place(x, q, z, h, k), place(*move(x, q, z, h, k))))
    return found


def send(value, move):
    return lax.ppermute(value, AXES, pairs(move))


def swap_core(value):
    return send(value, lambda x, q, z, h, k: (x, q, z, h, 1 - k))


def swap_q(value):
    return send(value, lambda x, q, z, h, k: (x, 1 - q, z, h, k))


def swap_h(value):
    return send(value, lambda x, q, z, h, k: (x, q, z, 1 - h, k))


def along_z(value, step):
    return send(value, lambda x, q, z, h, k: (x, q, (z + step) % 4, h, k))


def along_x(value, step):
    return send(value, lambda x, q, z, h, k: ((x + step) % 4, q, z, h, k))


def to_owner(value, step):
    return send(value, lambda x, q, z, h, k: ((x + z + step) % 4, h, x, q, k))


def turn_kernel(where_ref, own_ref, got_ref, *refs):
    outs, scratch = refs[:4], refs[4]
    own, got = own_ref[...], got_ref[...]
    first = where_ref[0] == 0
    both = jnp.concatenate([jnp.where(first, own, got), jnp.where(first, got, own)], axis=0)
    scratch[...] = both.T
    for step in range(4):
        start = pl.multiple_of(((where_ref[1] + step) % 4) * CHUNK, 32)
        outs[step][...] = scratch[pl.ds(start, CHUNK), :]


def turn(where, turned, got):
    width, rows = got.shape
    return pl.pallas_call(
        turn_kernel,
        out_shape=[jax.ShapeDtypeStruct((CHUNK, 2 * width), got.dtype)] * 4,
        grid_spec=pltpu.PrefetchScalarGridSpec(
            num_scalar_prefetch=1,
            grid=(1,),
            in_specs=[
                pl.BlockSpec((width, rows), lambda i, where: (0, where[0])),
                pl.BlockSpec((width, rows), lambda i, where: (0, 0)),
            ],
            out_specs=[pl.BlockSpec((CHUNK, 2 * width), lambda i, where: (0, 0))] * 4,
            scratch_shapes=[pltpu.VMEM((rows, 2 * width), got.dtype)],
        ),
        compiler_params=pltpu.CompilerParams(vmem_limit_bytes=16 << 20),
        name="turn",
    )(where, turned, got)


def laid(spots):
    def kernel(where_ref, *refs):
        count = len(spots)
        blocks, stages = refs[:count], refs[-count - 2 : -2]
        out_ref, into, out_of = refs[-count - 3], refs[-2], refs[-1]
        loads = [
            pltpu.make_async_copy(block, stage, into.at[i]) for i, (block, stage) in enumerate(zip(blocks, stages))
        ]
        for load in loads:
            load.start()
        stores = []
        for load, stage, (dx, other, steps) in zip(loads, stages, spots):
            load.wait()
            source = (where_ref[0] + dx) % 4
            for at, step in enumerate(steps):
                h = (where_ref[1] + other) % 2
                column = ((source - where_ref[2] - step + 8) % 4 * 2 + h) * 640
                row = source * CHUNK
                store = pltpu.make_async_copy(
                    stage.at[at],
                    out_ref.at[pl.ds(pl.multiple_of(row, 32), CHUNK), pl.ds(pl.multiple_of(column, 128), 640)],
                    out_of.at[len(stores)],
                )
                store.start()
                stores.append(store)
        for store in stores:
            store.wait()

    return kernel


def lay(where, blocks, spots, into=None):
    count = sum(len(spot[2]) for spot in spots)
    anywhere = pl.BlockSpec(memory_space=pl.ANY)
    operands = list(blocks) + ([] if into is None else [into])
    return pl.pallas_call(
        laid(spots),
        out_shape=jax.ShapeDtypeStruct((4 * CHUNK, 5120), blocks[0].dtype),
        grid_spec=pltpu.PrefetchScalarGridSpec(
            num_scalar_prefetch=1,
            grid=(1,),
            in_specs=[anywhere] * len(operands),
            out_specs=anywhere,
            scratch_shapes=[pltpu.VMEM(block.shape, block.dtype) for block in blocks]
            + [pltpu.SemaphoreType.DMA((len(blocks),)), pltpu.SemaphoreType.DMA((count,))],
        ),
        input_output_aliases={} if into is None else {len(operands): 0},
        compiler_params=pltpu.CompilerParams(vmem_limit_bytes=8 << 20),
    )(where, *operands)


def first_moves(new_weight):
    rows = new_weight.shape[0] // 2
    x, z, core = lax.axis_index("x"), lax.axis_index("z"), lax.axis_index("k")
    turned = new_weight.T
    other = lax.dynamic_slice(turned, (0, (1 - core) * rows), (turned.shape[0], rows))
    chunks = turn(jnp.stack([core, x + z]).astype(jnp.int32), turned, swap_core(other))
    got = [to_owner(chunks[step], step) for step in range(4)]
    return jnp.stack(got[:2]), jnp.stack(got[2:])


def move_weight(na, nb):
    x, q, z = lax.axis_index("x"), lax.axis_index("q"), lax.axis_index("z")
    fa, fb = swap_q(na), swap_q(nb)
    na_m, na_p = along_x(na, 1), along_x(na, -1)
    nb_m, nb_p = along_x(nb, 1), along_x(nb, -1)
    na_2, nb_2 = along_x(na_m, 1), along_x(nb_p, -1)
    fa_m, fa_p = along_x(fa, 1), along_x(fa, -1)
    fb_m, fb_p = along_x(fb, 1), along_x(fb, -1)
    fa_2, fb_2 = swap_q(na_2), swap_q(nb_2)
    a, b = (0, 1), (2, 3)
    where = jnp.stack([x, q, z]).astype(jnp.int32)
    out = None
    for spots in (
        [(na, 0, 0, a), (nb, 0, 0, b), (na_m, 3, 0, a), (na_p, 1, 0, a), (na_2, 2, 0, a), (fa, 0, 1, a)],
        [(nb_m, 3, 0, b), (nb_p, 1, 0, b), (fa_m, 3, 1, a), (fa_p, 1, 1, a), (fb, 0, 1, b)],
        [(nb_2, 2, 0, b), (fa_2, 2, 1, a), (fb_m, 3, 1, b), (fb_p, 1, 1, b), (fb_2, 2, 1, b)],
    ):
        out = lay(where, [spot[0] for spot in spots], [spot[1:] for spot in spots], out)
    return out


def stats_kernel(ids_ref, near_ref, far_ref, weight_ref, out_ref, rows_ref, sems):
    step = pl.program_id(0)
    half = near_ref.shape[0]

    @pl.when(step == 0)
    def _():
        copies = [
            pltpu.make_async_copy(near_ref, rows_ref.at[pl.ds(0, half)], sems.at[0]),
            pltpu.make_async_copy(far_ref, rows_ref.at[pl.ds(half, half)], sems.at[1]),
        ]
        for copy in copies:
            copy.start()
        for copy in copies:
            copy.wait()

    logits = lax.dot_general(
        weight_ref[...], rows_ref[...], (((1,), (1,)), ((), ())), preferred_element_type=jnp.float32
    )
    ids = lax.broadcasted_iota(jnp.int32, logits.shape, 0) + step * logits.shape[0]
    found = jnp.sum(jnp.where(ids == ids_ref[...], logits, 0.0), axis=0, keepdims=True)
    top = jnp.max(logits, axis=0, keepdims=True)

    @pl.when(step == 0)
    def _():
        out_ref[0:1] = top
        out_ref[1:2] = jnp.sum(jnp.exp(logits - top), axis=0, keepdims=True)
        out_ref[2:3] = found

    @pl.when(step > 0)
    def _():
        before = out_ref[0:1]
        highest = jnp.maximum(before, top)
        summed = jnp.sum(jnp.exp(logits - highest), axis=0, keepdims=True)
        out_ref[0:1] = highest
        out_ref[1:2] = out_ref[1:2] * jnp.exp(before - highest) + summed
        out_ref[2:3] = out_ref[2:3] + found


def row_stats(near, far, weight, ids):
    half, width = near.shape
    anywhere = pl.BlockSpec(memory_space=pl.ANY)
    return pl.pallas_call(
        stats_kernel,
        out_shape=jax.ShapeDtypeStruct((3, 2 * half), jnp.float32),
        grid=(weight.shape[0] // TILE,),
        in_specs=[
            pl.BlockSpec((1, 2 * half), lambda i: (0, 0)),
            anywhere,
            anywhere,
            pl.BlockSpec((TILE, width), lambda i: (i, 0)),
        ],
        out_specs=pl.BlockSpec((3, 2 * half), lambda i: (0, 0)),
        scratch_shapes=[pltpu.VMEM((2 * half, width), near.dtype), pltpu.SemaphoreType.DMA((2,))],
        compiler_params=pltpu.CompilerParams(vmem_limit_bytes=STATS_VMEM << 20),
        name="stats",
    )(ids.reshape(1, 2 * half), near, far, weight)


def cat_kernel(*refs):
    blocks, out_ref, stage, sems = refs[:-3], refs[-3], refs[-2], refs[-1]
    rows = blocks[0].shape[0]
    loads = [
        pltpu.make_async_copy(block, stage.at[pl.ds(i * rows, rows)], sems.at[i]) for i, block in enumerate(blocks)
    ]
    for load in loads:
        load.start()
    for load in loads:
        load.wait()
    store = pltpu.make_async_copy(stage, out_ref, sems.at[len(blocks)])
    store.start()
    store.wait()


def cat(blocks):
    shape = (len(blocks) * blocks[0].shape[0], blocks[0].shape[1])
    anywhere = pl.BlockSpec(memory_space=pl.ANY)
    return pl.pallas_call(
        cat_kernel,
        out_shape=jax.ShapeDtypeStruct(shape, blocks[0].dtype),
        in_specs=[anywhere] * len(blocks),
        out_specs=anywhere,
        scratch_shapes=[pltpu.VMEM(shape, blocks[0].dtype), pltpu.SemaphoreType.DMA((len(blocks) + 1,))],
        compiler_params=pltpu.CompilerParams(vmem_limit_bytes=8 << 20),
    )(*blocks)


def by_owner(stats):
    z, h, k = lax.axis_index("z"), lax.axis_index("h"), lax.axis_index("k")
    stats = stats[::-1]
    stats = jnp.concatenate([stats, stats], axis=0)
    stats = lax.dynamic_slice_in_dim(stats, (3 - z) % 4, 4, axis=0)
    stats = jnp.where(h == 0, stats, stats[:, ::-1])
    return jnp.where(k == 0, stats, stats[:, :, ::-1])


def relative(owned):
    z, h, k = lax.axis_index("z"), lax.axis_index("h"), lax.axis_index("k")
    owned = jnp.where(k == 0, owned, owned[:, :, ::-1])
    owned = jnp.where(h == 0, owned, owned[:, ::-1])
    owned = owned[::-1]
    owned = jnp.concatenate([owned, owned], axis=0)
    return lax.dynamic_slice_in_dim(owned, (3 - z) % 4, 4, axis=0)


def log_probs(hidden, tokens, old_weight):
    own_rows = hidden.shape[0]
    rank = (lax.axis_index("z") * 2 + lax.axis_index("h")) * 2 + lax.axis_index("k")
    wanted = relative(tokens.reshape(4, 2, 2, own_rows)) - rank * old_weight.shape[0]
    m, p = along_z(hidden, 1), along_z(hidden, -1)
    flipped = swap_h(hidden)
    far = along_z(m, 1)
    near = [hidden, m, far, p]
    m, p = along_z(flipped, 1), along_z(flipped, -1)
    far = along_z(p, -1)
    near = cat(near + [flipped, m, far, p])
    far = swap_core(near)
    ids = wanted.transpose(2, 1, 0, 3)
    stats = row_stats(near, far, old_weight, ids).reshape((3,) + ids.shape).transpose(3, 2, 1, 0, 4)
    stats = by_owner(stats).reshape(16, 3 * own_rows)
    stats = lax.all_to_all(stats, ("z", "h", "k"), split_axis=0, concat_axis=0, tiled=True)
    stats = stats.reshape(16, 3, own_rows)
    highest = jnp.max(stats[:, 0], axis=0)
    summed = jnp.sum(stats[:, 1] * jnp.exp(stats[:, 0] - highest[None, :]), axis=0)
    target = jnp.sum(stats[:, 2], axis=0)
    return target - highest - jnp.log(summed)


def on_device(hidden, tokens, old_weight, new_weight):
    na, nb = first_moves(new_weight)
    return log_probs(hidden, tokens, old_weight), move_weight(na, nb)


def solution(mesh):
    finer = Mesh(mesh.devices.reshape(SIZES), AXES)
    return jax.shard_map(
        on_device,
        mesh=finer,
        in_specs=(P(AXES, None), P(("x", "q")), P(("z", "h", "k"), None), P(("x", "q"), ("z", "h", "k"))),
        out_specs=(P(AXES), P(("z", "h", "k"), None)),
        check_vma=False,
    )
```

```python
import jax
import jax.numpy as jnp
from jax import lax
from jax.experimental import pallas as pl
from jax.experimental.pallas import tpu as pltpu
from jax.sharding import Mesh
from jax.sharding import PartitionSpec as P

AXES = ("x", "q", "z", "h", "k")
SIZES = (4, 2, 4, 2, 2)
TILE = 384
TILE = 384
STATS_VMEM = 56
CHUNK = 288


def place(x, q, z, h, k):
    return (((x * 2 + q) * 4 + z) * 2 + h) * 2 + k


def pairs(move):
    found = []
    for x in range(4):
        for q in range(2):
            for z in range(4):
                for h in range(2):
                    for k in range(2):
                        found.append((place(x, q, z, h, k), place(*move(x, q, z, h, k))))
    return found


def send(value, move):
    return lax.ppermute(value, AXES, pairs(move))


def swap_core(value):
    return send(value, lambda x, q, z, h, k: (x, q, z, h, 1 - k))


def swap_q(value):
    return send(value, lambda x, q, z, h, k: (x, 1 - q, z, h, k))


def swap_h(value):
    return send(value, lambda x, q, z, h, k: (x, q, z, 1 - h, k))


def along_z(value, step):
    return send(value, lambda x, q, z, h, k: (x, q, (z + step) % 4, h, k))


def along_x(value, step):
    return send(value, lambda x, q, z, h, k: ((x + step) % 4, q, z, h, k))


def to_owner(value, step):
    return send(value, lambda x, q, z, h, k: ((x + z + step) % 4, h, x, q, k))


def turn_kernel(where_ref, own_ref, got_ref, *refs):
    outs, scratch = refs[:4], refs[4]
    own, got = own_ref[...], got_ref[...]
    first = where_ref[0] == 0
    both = jnp.concatenate([jnp.where(first, own, got), jnp.where(first, got, own)], axis=0)
    scratch[...] = both.T
    for step in range(4):
        start = pl.multiple_of(((where_ref[1] + step) % 4) * CHUNK, 32)
        outs[step][...] = scratch[pl.ds(start, CHUNK), :]


def turn(where, turned, got):
    width, rows = got.shape
    return pl.pallas_call(
        turn_kernel,
        out_shape=[jax.ShapeDtypeStruct((CHUNK, 2 * width), got.dtype)] * 4,
        grid_spec=pltpu.PrefetchScalarGridSpec(
            num_scalar_prefetch=1,
            grid=(1,),
            in_specs=[
                pl.BlockSpec((width, rows), lambda i, where: (0, where[0])),
                pl.BlockSpec((width, rows), lambda i, where: (0, 0)),
            ],
            out_specs=[pl.BlockSpec((CHUNK, 2 * width), lambda i, where: (0, 0))] * 4,
            scratch_shapes=[pltpu.VMEM((rows, 2 * width), got.dtype)],
        ),
        compiler_params=pltpu.CompilerParams(vmem_limit_bytes=16 << 20),
        name="turn",
    )(where, turned, got)


def laid(spots):
    def kernel(where_ref, *refs):
        count = len(spots)
        blocks, stages = refs[:count], refs[-count - 2 : -2]
        out_ref, into, out_of = refs[-count - 3], refs[-2], refs[-1]
        loads = [
            pltpu.make_async_copy(block, stage, into.at[i]) for i, (block, stage) in enumerate(zip(blocks, stages))
        ]
        for load in loads:
            load.start()
        stores = []
        for load, stage, (dx, other, steps) in zip(loads, stages, spots):
            load.wait()
            source = (where_ref[0] + dx) % 4
            for at, step in enumerate(steps):
                h = (where_ref[1] + other) % 2
                column = ((source - where_ref[2] - step + 8) % 4 * 2 + h) * 640
                row = source * CHUNK
                store = pltpu.make_async_copy(
                    stage.at[at],
                    out_ref.at[pl.ds(pl.multiple_of(row, 32), CHUNK), pl.ds(pl.multiple_of(column, 128), 640)],
                    out_of.at[len(stores)],
                )
                store.start()
                stores.append(store)
        for store in stores:
            store.wait()

    return kernel


def lay(where, blocks, spots, into=None):
    count = sum(len(spot[2]) for spot in spots)
    anywhere = pl.BlockSpec(memory_space=pl.ANY)
    operands = list(blocks) + ([] if into is None else [into])
    return pl.pallas_call(
        laid(spots),
        out_shape=jax.ShapeDtypeStruct((4 * CHUNK, 5120), blocks[0].dtype),
        grid_spec=pltpu.PrefetchScalarGridSpec(
            num_scalar_prefetch=1,
            grid=(1,),
            in_specs=[anywhere] * len(operands),
            out_specs=anywhere,
            scratch_shapes=[pltpu.VMEM(block.shape, block.dtype) for block in blocks]
            + [pltpu.SemaphoreType.DMA((len(blocks),)), pltpu.SemaphoreType.DMA((count,))],
        ),
        input_output_aliases={} if into is None else {len(operands): 0},
        compiler_params=pltpu.CompilerParams(vmem_limit_bytes=8 << 20),
    )(where, *operands)


def first_moves(new_weight):
    rows = new_weight.shape[0] // 2
    x, z, core = lax.axis_index("x"), lax.axis_index("z"), lax.axis_index("k")
    turned = new_weight.T
    other = lax.dynamic_slice(turned, (0, (1 - core) * rows), (turned.shape[0], rows))
    chunks = turn(jnp.stack([core, x + z]).astype(jnp.int32), turned, swap_core(other))
    got = [to_owner(chunks[step], step) for step in range(4)]
    return jnp.stack(got)


def move_weight(n):
    x, q, z = lax.axis_index("x"), lax.axis_index("q"), lax.axis_index("z")
    f = swap_q(n)
    n_m, n_p = along_x(n, 1), along_x(n, -1)
    na_2, nb_2 = along_x(n_m[:2], 1), along_x(n_p[2:], -1)
    f_m, f_p = along_x(f, 1), along_x(f, -1)
    fa_2, fb_2 = swap_q(na_2), swap_q(nb_2)
    a, b, ab = (0, 1), (2, 3), (0, 1, 2, 3)
    where = jnp.stack([x, q, z]).astype(jnp.int32)
    out = None
    for spots in (
        [(n, 0, 0, ab), (n_m, 3, 0, ab), (n_p, 1, 0, ab), (f, 0, 1, ab)],
        [(na_2, 2, 0, a), (nb_2, 2, 0, b), (fa_2, 2, 1, a), (fb_2, 2, 1, b)],
        [(f_m, 3, 1, ab), (f_p, 1, 1, ab)],
    ):
        out = lay(where, [spot[0] for spot in spots], [spot[1:] for spot in spots], out)
    return out


def stats_kernel(ids_ref, hidden_ref, weight_ref, out_ref, rows_ref, sem):
    step = pl.program_id(0)

    @pl.when(step == 0)
    def _():
        copy = pltpu.make_async_copy(hidden_ref, rows_ref, sem)
        copy.start()
        copy.wait()

    logits = lax.dot_general(
        weight_ref[...], rows_ref[...], (((1,), (1,)), ((), ())), preferred_element_type=jnp.float32
    )
    ids = lax.broadcasted_iota(jnp.int32, logits.shape, 0) + step * logits.shape[0]
    found = jnp.sum(jnp.where(ids == ids_ref[...], logits, 0.0), axis=0, keepdims=True)
    top = jnp.max(logits, axis=0, keepdims=True)

    @pl.when(step == 0)
    def _():
        out_ref[0:1] = top
        out_ref[1:2] = jnp.sum(jnp.exp(logits - top), axis=0, keepdims=True)
        out_ref[2:3] = found

    @pl.when(step > 0)
    def _():
        before = out_ref[0:1]
        highest = jnp.maximum(before, top)
        summed = jnp.sum(jnp.exp(logits - highest), axis=0, keepdims=True)
        out_ref[0:1] = highest
        out_ref[1:2] = out_ref[1:2] * jnp.exp(before - highest) + summed
        out_ref[2:3] = out_ref[2:3] + found


def row_stats(rows, weight, ids):
    count, width = rows.shape
    return pl.pallas_call(
        stats_kernel,
        out_shape=jax.ShapeDtypeStruct((3, count), jnp.float32),
        grid=(weight.shape[0] // TILE,),
        in_specs=[
            pl.BlockSpec((1, count), lambda i: (0, 0)),
            pl.BlockSpec(memory_space=pl.ANY),
            pl.BlockSpec((TILE, width), lambda i: (i, 0)),
        ],
        out_specs=pl.BlockSpec((3, count), lambda i: (0, 0)),
        scratch_shapes=[pltpu.VMEM((count, width), rows.dtype), pltpu.SemaphoreType.DMA(())],
        compiler_params=pltpu.CompilerParams(vmem_limit_bytes=STATS_VMEM << 20),
    )(ids.reshape(1, count), rows, weight)


def cat_kernel(*refs):
    blocks, out_ref, stage, sems = refs[:-3], refs[-3], refs[-2], refs[-1]
    rows = blocks[0].shape[0]
    loads = [
        pltpu.make_async_copy(block, stage.at[pl.ds(i * rows, rows)], sems.at[i]) for i, block in enumerate(blocks)
    ]
    for load in loads:
        load.start()
    for load in loads:
        load.wait()
    store = pltpu.make_async_copy(stage, out_ref, sems.at[len(blocks)])
    store.start()
    store.wait()


def cat(blocks):
    shape = (len(blocks) * blocks[0].shape[0], blocks[0].shape[1])
    anywhere = pl.BlockSpec(memory_space=pl.ANY)
    return pl.pallas_call(
        cat_kernel,
        out_shape=jax.ShapeDtypeStruct(shape, blocks[0].dtype),
        in_specs=[anywhere] * len(blocks),
        out_specs=anywhere,
        scratch_shapes=[pltpu.VMEM(shape, blocks[0].dtype), pltpu.SemaphoreType.DMA((len(blocks) + 1,))],
        compiler_params=pltpu.CompilerParams(vmem_limit_bytes=8 << 20),
    )(*blocks)


def by_owner(stats):
    z, h, k = lax.axis_index("z"), lax.axis_index("h"), lax.axis_index("k")
    stats = stats[::-1]
    stats = jnp.concatenate([stats, stats], axis=0)
    stats = lax.dynamic_slice_in_dim(stats, (3 - z) % 4, 4, axis=0)
    stats = jnp.where(h == 0, stats, stats[:, ::-1])
    return jnp.where(k == 0, stats, stats[:, :, ::-1])


def relative(owned):
    z, h, k = lax.axis_index("z"), lax.axis_index("h"), lax.axis_index("k")
    owned = jnp.where(k == 0, owned, owned[:, :, ::-1])
    owned = jnp.where(h == 0, owned, owned[:, ::-1])
    owned = owned[::-1]
    owned = jnp.concatenate([owned, owned], axis=0)
    return lax.dynamic_slice_in_dim(owned, (3 - z) % 4, 4, axis=0)


def log_probs(hidden, tokens, old_weight):
    own_rows = hidden.shape[0]
    rank = (lax.axis_index("z") * 2 + lax.axis_index("h")) * 2 + lax.axis_index("k")
    wanted = relative(tokens.reshape(4, 2, 2, own_rows)) - rank * old_weight.shape[0]
    m, p = along_z(hidden, 1), along_z(hidden, -1)
    flipped = swap_h(hidden)
    far = along_z(m, 1)
    near = [hidden, m, far, p]
    m, p = along_z(flipped, 1), along_z(flipped, -1)
    far = along_z(p, -1)
    near = cat(near + [flipped, m, far, p])
    far = swap_core(near)
    ids = wanted.transpose(2, 1, 0, 3)
    stats = [row_stats(rows, old_weight, ids[flip]) for flip, rows in enumerate((near, far))]
    stats = jnp.stack(stats).reshape(2, 3, 2, 4, own_rows).transpose(3, 2, 0, 1, 4)
    stats = by_owner(stats).reshape(16, 3 * own_rows)
    stats = lax.all_to_all(stats, ("z", "h", "k"), split_axis=0, concat_axis=0, tiled=True)
    stats = stats.reshape(16, 3, own_rows)
    highest = jnp.max(stats[:, 0], axis=0)
    summed = jnp.sum(stats[:, 1] * jnp.exp(stats[:, 0] - highest[None, :]), axis=0)
    target = jnp.sum(stats[:, 2], axis=0)
    return target - highest - jnp.log(summed)


def on_device(hidden, tokens, old_weight, new_weight):
    n = first_moves(new_weight)
    return log_probs(hidden, tokens, old_weight), move_weight(n)


def solution(mesh):
    finer = Mesh(mesh.devices.reshape(SIZES), AXES)
    return jax.shard_map(
        on_device,
        mesh=finer,
        in_specs=(P(AXES, None), P(("x", "q")), P(("z", "h", "k"), None), P(("x", "q"), ("z", "h", "k"))),
        out_specs=(P(AXES), P(("z", "h", "k"), None)),
        check_vma=False,
    )
```
